128 devices in a mesh: row: 32 (over y, x, core), col: 4 (over z).
Axes of the slice: x: 4, y: 4, z: 4, core: 2. Of those that a mesh axis runs over, the one named last changes fastest.
Arguments:
- density: float32 [256, 256, 256], P('row', 'col'), may hold values from -5 to 5
- green_octant: float32 [256, 256, 256], P('row', 'col'), may hold values from 0 to 0.25
Outputs:
- potential: float32 [256, 256, 256], P('row', 'col')
The draws below stay inside these ranges and needn't reach their ends.
All inputs are finite; a program needn't handle non-finite values.
Results may differ from the reference program's by a relative error of at most 0.000092.
Values sent between devices are 32-bit elements; how exact they have to be, the bound alone decides.
A program may use at most 64 MiB of HBM per device.

```python
import math
import jax
import jax.numpy as jnp
from jax import lax

N = 256


def draw_density(key, part):
    noise = jax.random.normal(key, (N, N, N), jnp.float32)
    return jnp.clip(noise, -5.0, 5.0)


def draw_green_octant(key, part):
    coords = jnp.arange(N, dtype=jnp.float32)
    radius = jnp.sqrt(coords[:, None, None] * coords[:, None, None] + coords[None, :, None] * coords[None, :, None] + coords[None, None, :] * coords[None, None, :])
    factor = jnp.exp(jax.random.uniform(key, (N, N, N), jnp.float32, math.log(0.5), math.log(1.5)))
    return factor * jnp.exp(-radius / (N / 4.0)) / (4.0 * math.pi * jnp.maximum(radius, 0.5))


def setup_inputs(seed: int = 0) -> dict:
    streams_of = jax.random.split(jax.random.key(seed), 3)
    return {
        "density": draw_density(jax.random.fold_in(streams_of[2], 71), 0),
        "green_octant": draw_green_octant(jax.random.fold_in(streams_of[2], 71), 0),
    }


def cosine_table(extent, padded):
    positions = jnp.arange(extent, dtype=jnp.int32)[:, None]
    waves = jnp.arange(padded, dtype=jnp.int32)[None, :]
    phases = (positions * waves) % padded
    angles = phases.astype(jnp.float32) * jnp.float32(2.0 * 3.141592653589793 / padded)
    weights = jnp.where(positions == 0, jnp.float32(1.0), jnp.float32(2.0))
    return weights * jnp.cos(angles)


def reference(density, green_octant):
    padded = 2 * N
    table = cosine_table(N, padded)
    half_table = table[:, : N + 1]
    along_z = jnp.dot(green_octant.reshape(N * N, N), half_table, precision=lax.Precision.HIGHEST, preferred_element_type=jnp.float32).reshape(N, N, N + 1)
    along_y = jnp.einsum("ijk,jl->ilk", along_z, table, precision=lax.Precision.HIGHEST)
    kernel_hat = jnp.einsum("ijk,il->ljk", along_y, table, precision=lax.Precision.HIGHEST)
    density_hat = jnp.fft.rfftn(density, s=(padded, padded, padded))
    product = density_hat * kernel_hat
    whole = jnp.fft.irfftn(product, s=(padded, padded, padded))
    return whole[:N, :N, :N].astype(jnp.float32)
```

```python
import itertools

import jax
import jax.numpy as jnp
import numpy as np
from jax import lax
from jax.experimental import pallas as pl
from jax.experimental.pallas import tpu as pltpu
from jax.sharding import PartitionSpec as P

N = 256
ROWS, COLS = 32, 4
DEVICES = ROWS * COLS
BF16, F32 = jnp.bfloat16, jnp.float32
MESH = pl.DeviceIdType.MESH


def hops(offset):
    return sum(min(step, 4 - step) for step in (offset[0], offset[1], offset[3]))


OFFSETS = [o for o in itertools.product(range(4), range(4), range(2), range(4)) if any(o)]
OFFSETS.sort(key=lambda o: -hops(o))


def split(value):
    high = value.astype(BF16)
    return high, (value - high.astype(F32)).astype(BF16)


def tables():
    wave = np.arange(N)[:, None]
    cell = np.arange(N)[None, :]
    angle = np.pi * (((2 * wave + 1) * cell) % (4 * N)) / (2 * N)
    frame = np.concatenate([np.cos(angle), np.sin(angle)], axis=0)
    even = np.where(cell == 0, 1.0, 2.0) * np.cos(angle)
    out = []
    for table in (frame, frame.T, even, even.T):
        high = table.astype(np.float32).astype(BF16)
        out.append(high)
        out.append((table - high.astype(np.float64)).astype(np.float32).astype(BF16))
    return out


def dot3(a, b, dims=(((1,), (0,)), ((), ()))):
    def one(x, y):
        return lax.dot_general(x, y, dims, preferred_element_type=F32)

    return one(a[0], b[0]) + one(a[0], b[1]) + one(a[1], b[0])


def low_half(shape):
    return lax.broadcasted_iota(jnp.int32, shape, len(shape) - 1) < 64


def exchange_halves(a, b):
    low = low_half(a.shape)
    return (
        jnp.where(low, a, pltpu.roll(b, 64, 1)),
        jnp.where(low, pltpu.roll(a, 64, 1), b),
    )


def kernel(
    dens, green, th, tl, tth, ttl, wh, wl, wth, wtl, out,
    send_k, send_d, recv_k, recv_d, send_i, recv_i, khat, stage, total, send_sem, recv_sem,
):
    row, z = lax.axis_index("row"), lax.axis_index("col")
    y, x, c = row // 8, (row // 2) % 4, row % 2
    mine = z * ROWS + row

    def partners():
        for dy, dx, dc, dz in OFFSETS:
            r = (((y + dy) % 4) * 4 + (x + dx) % 4) * 2 + (c + dc) % 2
            yield r, (z + dz) % 4

    barrier = pltpu.get_barrier_semaphore()
    for r, q in partners():
        pl.semaphore_signal(barrier, inc=1, device_id=(r, q), device_id_type=MESH)

    def tile(ref, slot):
        return ref.at[pl.ds(pl.multiple_of(slot * 8, 8), 8)]

    def send(source, target, index):
        for r, q in partners():
            pltpu.make_async_remote_copy(
                src_ref=tile(source, q * ROWS + r),
                dst_ref=tile(target, mine),
                send_sem=send_sem.at[index],
                recv_sem=recv_sem.at[index],
                device_id=(r, q),
                device_id_type=MESH,
            ).start()
        own = pl.ds(pl.multiple_of(mine * 8, 8), 8)
        target[own, :] = source[own, :]

    def arrived(target, sem):
        most = target.at[pl.ds(0, (DEVICES - 1) * 8)]
        pltpu.make_async_copy(most, most, sem).wait()

    def along_z(table, data, target):
        nt = (((1,), (1,)), ((), ()))
        for t in range(4):
            part = (data[0][128 * t : 128 * t + 128], data[1][128 * t : 128 * t + 128])
            result = dot3(table, part, nt)
            first, second = exchange_halves(result[:128], result[128:])
            target[pl.ds(2 * t, DEVICES, stride=8), :] = first
            target[pl.ds(2 * t + 1, DEVICES, stride=8), :] = second

    def both(high, low, start):
        return tuple(
            jnp.concatenate([r[start : start + 128], r[N + start : N + start + 128]], 0)
            for r in (high, low)
        )

    g = split(green[...].reshape(8 * 64, N))
    along_z((wh[...], wl[...]), g, send_k)
    d = split(dens[...].reshape(8 * 64, N))
    along_z(both(th, tl, 0), d, send_d.at[0])
    pl.semaphore_wait(barrier, DEVICES - 1)
    send(send_k, recv_k, 0)
    send(send_d.at[0], recv_d.at[0], 1)
    along_z(both(th, tl, 128), d, send_d.at[1])
    send(send_d.at[1], recv_d.at[1], 2)

    def planes(ref):
        first, second = [], []
        for t in range(2):
            a = ref[512 * t : 512 * t + 256, :]
            b = ref[512 * t + 256 : 512 * t + 512, :]
            low, high = exchange_halves(a, b)
            first.append(low)
            second.append(high)
        return jnp.concatenate(first, 1), jnp.concatenate(second, 1)

    arrived(recv_k, recv_sem.at[0])
    for half, plane in enumerate(planes(recv_k)):
        along_y = dot3(split(plane), (wth[...], wtl[...]))
        khat[half] = dot3((wh[...], wl[...]), split(along_y)) * F32(1.0 / N**3)

    for half in range(2):
        arrived(recv_d.at[half], recv_sem.at[1 + half])
        done = []
        for plane in planes(recv_d.at[half]):
            along_y = dot3(split(plane), (tth[...], ttl[...]))
            along_x = dot3((th[...], tl[...]), split(along_y))
            k = khat[half]
            k = jnp.concatenate([k, k], 1)
            along_x = along_x * jnp.concatenate([k, k], 0)
            back_x = dot3((tth[...], ttl[...]), split(along_x))
            done.append(dot3(split(back_x), (th[...], tl[...])))
        target = send_i.at[half]
        for t in range(2):
            lanes = slice(128 * t, 128 * t + 128)
            low, high = exchange_halves(done[0][:, lanes], done[1][:, lanes])
            target[512 * t : 512 * t + 256, :] = low
            target[512 * t + 256 : 512 * t + 512, :] = high
        send(target, recv_i.at[half], 3 + half)

    for half in range(2):
        arrived(recv_i.at[half], recv_sem.at[3 + half])
        source = recv_i.at[half]
        table = tuple(
            jnp.concatenate(
                [r[:, 128 * half : 128 * half + 128], r[:, N + 128 * half : N + 128 * half + 128]], 1
            )
            for r in (tth, ttl)
        )
        for t in range(4):
            a = source[pl.ds(2 * t, DEVICES, stride=8), :]
            b = source[pl.ds(2 * t + 1, DEVICES, stride=8), :]
            first, second = exchange_halves(a, b)
            waves = split(jnp.concatenate([first, second], 0))
            part = dot3(table, waves)
            if half == 0:
                total[:, 128 * t : 128 * t + 128] = part
            else:
                part = part + total[:, 128 * t : 128 * t + 128]
                out[2 * t : 2 * t + 2] = part.T.reshape(2, 64, N)

    for index, ref in enumerate([recv_k, recv_d.at[0], recv_d.at[1], recv_i.at[0], recv_i.at[1]]):
        arrived(ref, send_sem.at[index])


def solution(mesh):
    constants = tables()

    def on_device(density, green_octant):
        vmem = pl.BlockSpec(memory_space=pltpu.VMEM)
        one = pltpu.VMEM((DEVICES * 8, 128), F32)
        two = pltpu.VMEM((2, DEVICES * 8, 128), F32)
        return pl.pallas_call(
            kernel,
            out_shape=jax.ShapeDtypeStruct((8, 64, N), F32),
            in_specs=[vmem] * (2 + len(constants)),
            out_specs=vmem,
            scratch_shapes=[
                one, two, one, two, two, two,
                pltpu.VMEM((2, N, N), F32),
                pltpu.VMEM((8, 128), F32),
                pltpu.VMEM((N, 512), F32),
                pltpu.SemaphoreType.DMA((5,)),
                pltpu.SemaphoreType.DMA((5,)),
            ],
            compiler_params=pltpu.CompilerParams(
                collective_id=0, has_side_effects=True, vmem_limit_bytes=56 << 20
            ),
        )(density, green_octant, *[jnp.asarray(t) for t in constants])

    return jax.shard_map(
        on_device,
        mesh=mesh,
        in_specs=(P("row", "col", None), P("row", "col", None)),
        out_specs=P("row", "col", None),
        check_vma=False,
    )
```

```python
import itertools

import jax
import jax.numpy as jnp
import numpy as np
from jax import lax
from jax.experimental import pallas as pl
from jax.experimental.pallas import tpu as pltpu
from jax.sharding import PartitionSpec as P

N = 256
ROWS, COLS = 32, 4
DEVICES = ROWS * COLS
BF16, F32 = jnp.bfloat16, jnp.float32
MESH = pl.DeviceIdType.MESH
DENS, GREEN, TH, TL, TTH, TTL, WH, WL, WTH, WTL = range(10)


def hops(offset):
    return sum(min(step, 4 - step) for step in (offset[0], offset[1], offset[3]))


OFFSETS = [o for o in itertools.product(range(4), range(4), range(2), range(4)) if any(o)]
OFFSETS.sort(key=lambda o: -hops(o))


def split(value):
    high = value.astype(BF16)
    return high, (value - high.astype(F32)).astype(BF16)


def tables():
    wave = np.arange(N)[:, None]
    cell = np.arange(N)[None, :]
    angle = np.pi * (((2 * wave + 1) * cell) % (4 * N)) / (2 * N)
    frame = np.concatenate([np.cos(angle), np.sin(angle)], axis=0)
    even = np.where(cell == 0, 1.0, 2.0) * np.cos(angle)
    out = []
    for table in (frame, frame.T, even, even.T):
        high = table.astype(np.float32).astype(BF16)
        out.append(high)
        out.append((table - high.astype(np.float64)).astype(np.float32).astype(BF16))
    return out


def dot3(a, b, dims=(((1,), (0,)), ((), ()))):
    def one(x, y):
        return lax.dot_general(x, y, dims, preferred_element_type=F32)

    return one(a[0], b[0]) + one(a[0], b[1]) + one(a[1], b[0])


def low_half(shape):
    return lax.broadcasted_iota(jnp.int32, shape, len(shape) - 1) < 64


def exchange_halves(a, b):
    low = low_half(a.shape)
    return (
        jnp.where(low, a, pltpu.roll(b, 64, 1)),
        jnp.where(low, pltpu.roll(a, 64, 1), b),
    )


def kernel(*refs):
    operands, out, refs = refs[:10], refs[10], refs[11:]
    fetched, refs = refs[:10], refs[10:]
    send_f, recv_f, send_i, recv_i, khat, stage, total, send_sem, recv_sem, load_sem = refs
    dens, green, th, tl, tth, ttl, wh, wl, wth, wtl = fetched
    row, z = lax.axis_index("row"), lax.axis_index("col")
    y, x, c = row // 8, (row // 2) % 4, row % 2
    mine = z * ROWS + row

    def partners():
        for dy, dx, dc, dz in OFFSETS:
            r = (((y + dy) % 4) * 4 + (x + dx) % 4) * 2 + (c + dc) % 2
            yield r, (z + dz) % 4

    barrier = pltpu.get_barrier_semaphore()
    def load(index):
        return pltpu.make_async_copy(operands[index], fetched[index], load_sem.at[index])

    order = (DENS, TH, TL, GREEN, WH, WL, WTH, WTL, TTH, TTL)
    for index in order[:3]:
        load(index).start()
    for r, q in partners():
        pl.semaphore_signal(barrier, inc=1, device_id=(r, q), device_id_type=MESH)
    for index in order[3:]:
        load(index).start()

    def tile(ref, slot):
        return ref.at[pl.ds(pl.multiple_of(slot * 8, 8), 8)]

    def send(source, target, index):
        for r, q in partners():
            pltpu.make_async_remote_copy(
                src_ref=tile(source, q * ROWS + r),
                dst_ref=tile(target, mine),
                send_sem=send_sem.at[index],
                recv_sem=recv_sem.at[index],
                device_id=(r, q),
                device_id_type=MESH,
            ).start()
        own = pl.ds(pl.multiple_of(mine * 8, 8), 8)
        target[own, :] = source[own, :]

    def arrived(target, sem):
        most = target.at[pl.ds(0, (DEVICES - 1) * 8)]
        pltpu.make_async_copy(most, most, sem).wait()

    def along_z(upper, lower, target):
        def one(pair, t):
            rows = slice(128 * t, 128 * t + 128)
            data = tuple(ref[rows] for ref in pair[1])
            return dot3(pair[0], data, (((1,), (1,)), ((), ())))

        for t in range(4):
            first, second = exchange_halves(one(upper, t), one(lower, t))
            target[pl.ds(2 * t, DEVICES, stride=8), :] = first
            target[pl.ds(2 * t + 1, DEVICES, stride=8), :] = second

    def rows_of(high, low, start):
        return high[start : start + 128], low[start : start + 128]

    for index in order[:6]:
        load(index).wait()
    g = split(green[...].reshape(8 * 64, N))
    d = split(dens[...].reshape(8 * 64, N))
    along_z((rows_of(th, tl, 0), d), (rows_of(wh, wl, 0), g), send_f.at[0])
    pl.semaphore_wait(barrier, DEVICES - 1)
    send(send_f.at[0], recv_f.at[0], 0)
    along_z((rows_of(th, tl, N), d), (rows_of(wh, wl, 128), g), send_f.at[1])
    send(send_f.at[1], recv_f.at[1], 1)
    along_z((rows_of(th, tl, 128), d), (rows_of(th, tl, N + 128), d), send_f.at[2])
    send(send_f.at[2], recv_f.at[2], 2)
    for index in order[6:]:
        load(index).wait()

    def planes(ref):
        first, second = [], []
        for t in range(2):
            a = ref[512 * t : 512 * t + 256, :]
            b = ref[512 * t + 256 : 512 * t + 512, :]
            low, high = exchange_halves(a, b)
            first.append(low)
            second.append(high)
        return jnp.concatenate(first, 1), jnp.concatenate(second, 1)

    def transform_kernel(half, plane):
        along_y = dot3(split(plane), (wth[...], wtl[...]))
        khat[half] = dot3((wh[...], wl[...]), split(along_y)) * F32(1.0 / N**3)

    def convolve(half, plane):
        along_y = dot3(split(plane), (tth[...], ttl[...]))
        along_x = dot3((th[...], tl[...]), split(along_y))
        k = khat[half]
        k = jnp.concatenate([k, k], 1)
        along_x = along_x * jnp.concatenate([k, k], 0)
        back_x = dot3((tth[...], ttl[...]), split(along_x))
        return dot3(split(back_x), (th[...], tl[...]))

    def send_back(half, cosine, sine):
        target = send_i.at[half]
        for t in range(2):
            lanes = slice(128 * t, 128 * t + 128)
            low, high = exchange_halves(cosine[:, lanes], sine[:, lanes])
            target[512 * t : 512 * t + 256, :] = low
            target[512 * t + 256 : 512 * t + 512, :] = high
        send(target, recv_i.at[half], 3 + half)

    arrived(recv_f.at[0], recv_sem.at[0])
    plane, plane_k = planes(recv_f.at[0])
    transform_kernel(0, plane_k)
    stage[...] = convolve(0, plane)
    arrived(recv_f.at[1], recv_sem.at[1])
    plane, plane_k = planes(recv_f.at[1])
    send_back(0, stage[...], convolve(0, plane))
    transform_kernel(1, plane_k)
    arrived(recv_f.at[2], recv_sem.at[2])
    plane, other = planes(recv_f.at[2])
    send_back(1, convolve(1, plane), convolve(1, other))

    for half in range(2):
        arrived(recv_i.at[half], recv_sem.at[3 + half])
        source = recv_i.at[half]
        table = tuple(
            jnp.concatenate(
                [r[:, 128 * half : 128 * half + 128], r[:, N + 128 * half : N + 128 * half + 128]], 1
            )
            for r in (tth, ttl)
        )
        for t in range(4):
            a = source[pl.ds(2 * t, DEVICES, stride=8), :]
            b = source[pl.ds(2 * t + 1, DEVICES, stride=8), :]
            first, second = exchange_halves(a, b)
            waves = split(jnp.concatenate([first, second], 0))
            part = dot3(table, waves)
            if half == 0:
                total[:, 128 * t : 128 * t + 128] = part
            else:
                part = part + total[:, 128 * t : 128 * t + 128]
                out[2 * t : 2 * t + 2] = part.T.reshape(2, 64, N)

    for index in range(5):
        arrived(recv_i.at[0], send_sem.at[index])


def solution(mesh):
    constants = tables()

    def on_device(density, green_octant):
        vmem = pl.BlockSpec(memory_space=pltpu.VMEM)
        operands = [density, green_octant, *[jnp.asarray(t) for t in constants]]
        three = pltpu.VMEM((3, DEVICES * 8, 128), F32)
        two = pltpu.VMEM((2, DEVICES * 8, 128), F32)
        return pl.pallas_call(
            kernel,
            out_shape=pltpu.VMEM((8, 64, N), F32),
            in_specs=[pl.BlockSpec(memory_space=pl.ANY)] * len(operands),
            out_specs=vmem,
            scratch_shapes=[
                *[pltpu.VMEM(o.shape, o.dtype) for o in operands],
                three, three, two, two,
                pltpu.VMEM((2, N, N), F32),
                pltpu.VMEM((N, N), F32),
                pltpu.VMEM((N, 512), F32),
                pltpu.SemaphoreType.DMA((5,)),
                pltpu.SemaphoreType.DMA((5,)),
                pltpu.SemaphoreType.DMA((len(operands),)),
            ],
            compiler_params=pltpu.CompilerParams(
                collective_id=0, has_side_effects=True, vmem_limit_bytes=56 << 20
            ),
        )(*operands)

    return jax.shard_map(
        on_device,
        mesh=mesh,
        in_specs=(P("row", "col", None), P("row", "col", None)),
        out_specs=P("row", "col", None),
        check_vma=False,
    )
```

```python
import itertools
import random

import jax
import jax.numpy as jnp
import numpy as np
from jax import lax
from jax.experimental import pallas as pl
from jax.experimental.pallas import tpu as pltpu
from jax.sharding import PartitionSpec as P

N = 256
ROWS, COLS = 32, 4
DEVICES = ROWS * COLS
BF16, F32 = jnp.bfloat16, jnp.float32
MESH = pl.DeviceIdType.MESH
DENS, GREEN, TH, TL, TTH, TTL, WH, WL, WTH, WTL, XWH, XWL, XF, XFL, XIH, XIL = range(16)


def steps(offset):
    taken = np.zeros((3, 2))
    for dim, step in enumerate((offset[0], offset[1], offset[3])):
        if step == 2:
            taken[dim] += 1
        elif step:
            taken[dim, step // 2] += 1
    return taken


def send_order(seed, window=40):
    rest = [o for o in itertools.product(range(4), range(4), range(2), range(4)) if any(o)]
    random.Random(seed).shuffle(rest)
    rest.sort(key=lambda o: -sum(min(n, 4 - n) for n in (o[0], o[1], o[3])))
    load, order = np.zeros((3, 2)), []
    while rest:
        best = min(rest[:window], key=lambda o: ((load + steps(o)).max(), (load + steps(o)).var()))
        rest.remove(best)
        load += steps(best)
        order.append(best)
    return order


ORDERS = [send_order(5 + chunk) for chunk in range(5)]


def split(value):
    high = value.astype(BF16)
    return high, (value - high.astype(F32)).astype(BF16)


def tables():
    wave = np.arange(N)[:, None]
    cell = np.arange(N)[None, :]
    angle = np.pi * (((2 * wave + 1) * cell) % (4 * N)) / (2 * N)
    frame = np.concatenate([np.cos(angle), np.sin(angle)], axis=0)
    even = np.where(cell == 0, 1.0, 2.0) * np.cos(angle)
    folded = np.concatenate([np.arange(N // 2), np.arange(N - 1, N // 2 - 1, -1)])
    middle = np.pi * (((2 * wave + 1) * (2 * cell[:, : N // 2] - (N - 1))) % (8 * N)) / (4 * N)
    half = np.concatenate([np.cos(middle), np.sin(middle)], axis=0)

    def terms(table):
        high = table.astype(np.float32).astype(BF16)
        return [high, (table - high.astype(np.float64)).astype(np.float32).astype(BF16)]

    out = []
    for table in (frame, frame.T, even, even.T, even[:, folded]):
        out += terms(table)
    high, low = terms(half)
    out += [np.concatenate([high, high], axis=1), low]
    high, low = terms(np.concatenate([np.cos(middle).T, np.sin(middle).T], axis=1))
    return [*out, high, low]


def dot3(a, b, dims=(((1,), (0,)), ((), ()))):
    def one(x, y):
        return lax.dot_general(x, y, dims, preferred_element_type=F32)

    return one(a[0], b[0]) + one(a[0], b[1]) + one(a[1], b[0])


def low_half(shape):
    return lax.broadcasted_iota(jnp.int32, shape, len(shape) - 1) < 64


def exchange_halves(a, b):
    low = low_half(a.shape)
    return (
        jnp.where(low, a, pltpu.roll(b, 64, 1)),
        jnp.where(low, pltpu.roll(a, 64, 1), b),
    )


def kernel(*refs):
    operands, out, refs = refs[:16], refs[16], refs[17:]
    fetched, refs = refs[:16], refs[16:]
    send_f, recv_f, send_i, recv_i, khat, stage, waves, total, send_sem, recv_sem, load_sem = refs
    dens, green, th, tl, tth, ttl, wh, wl, wth, wtl, xwh, xwl, xf, xfl, xih, xil = fetched
    row, z = lax.axis_index("row"), lax.axis_index("col")
    y, x, c = row // 8, (row // 2) % 4, row % 2
    flip = row // 16

    def slot(r, q):
        return q * ROWS + r + (r // 16) * (47 - 2 * r)

    def line(n):
        return n + flip * (7 - 2 * n)

    mine = slot(row, z)

    def partners(chunk=0):
        for dy, dx, dc, dz in ORDERS[chunk]:
            r = (((y + dy) % 4) * 4 + (x + dx) % 4) * 2 + (c + dc) % 2
            yield r, (z + dz) % 4

    barrier = pltpu.get_barrier_semaphore()
    def load(index):
        return pltpu.make_async_copy(operands[index], fetched[index], load_sem.at[index])

    order = (DENS, TH, TL, GREEN, WH, WL, WTH, WTL, XWH, XWL, TTH, TTL, XF, XFL, XIH, XIL)
    for index in order[:3]:
        load(index).start()
    for r, q in partners():
        pl.semaphore_signal(barrier, inc=1, device_id=(r, q), device_id_type=MESH)
    for index in order[3:]:
        load(index).start()

    def tile(ref, index):
        return ref.at[pl.ds(pl.multiple_of(index * 8, 8), 8)]

    def send(source, target, index):
        for r, q in partners(index):
            pltpu.make_async_remote_copy(
                src_ref=tile(source, slot(r, q)),
                dst_ref=tile(target, mine),
                send_sem=send_sem.at[index],
                recv_sem=recv_sem.at[index],
                device_id=(r, q),
                device_id_type=MESH,
            ).start()
        own = pl.ds(pl.multiple_of(mine * 8, 8), 8)
        target[own, :] = source[own, :]

    def arrived(target, sem):
        most = target.at[pl.ds(0, (DEVICES - 1) * 8)]
        pltpu.make_async_copy(most, most, sem).wait()

    def along_z(upper, lower, target):
        def one(pair, t):
            rows = slice(128 * t, 128 * t + 128)
            data = tuple(ref[rows] for ref in pair[1])
            return dot3(pair[0], data, (((1,), (1,)), ((), ())))

        for t in range(4):
            first, second = exchange_halves(one(upper, t), one(lower, t))
            target[pl.ds(line(2 * t), DEVICES, stride=8), :] = first
            target[pl.ds(line(2 * t + 1), DEVICES, stride=8), :] = second

    def rows_of(high, low, start):
        return high[start : start + 128], low[start : start + 128]

    for index in order[:6]:
        load(index).wait()
    g = split(green[...].reshape(8 * 64, N))
    d = split(dens[...].reshape(8 * 64, N))
    along_z((rows_of(th, tl, 0), d), (rows_of(wh, wl, 0), g), send_f.at[0])
    pl.semaphore_wait(barrier, DEVICES - 1)
    send(send_f.at[0], recv_f.at[0], 0)
    along_z((rows_of(th, tl, N), d), (rows_of(th, tl, 128), d), send_f.at[1])
    send(send_f.at[1], recv_f.at[1], 1)
    along_z((rows_of(th, tl, N + 128), d), (rows_of(wh, wl, 128), g), send_f.at[2])
    send(send_f.at[2], recv_f.at[2], 2)
    for index in order[6:]:
        load(index).wait()

    def planes(ref):
        first, second = [], []
        for t in range(2):
            a = ref[512 * t : 512 * t + 256, :]
            b = ref[512 * t + 256 : 512 * t + 512, :]
            low, high = exchange_halves(a, b)
            first.append(low)
            second.append(high)
        return jnp.concatenate(first, 1), jnp.concatenate(second, 1)

    def transform_kernel(half, plane):
        along_y = dot3(split(plane), (wth[...], wtl[...]))
        khat[half] = dot3((xwh[...], xwl[...]), split(along_y)) * F32(1.0 / N**3)

    def ahead(plane):
        along_y = dot3(split(plane), (tth[...], ttl[...]))
        upper, lower = along_y[: N // 2], along_y[N // 2 :]

        def along_x(start, cells):
            high, low = split(cells)
            rows = slice(start, start + N)
            return jnp.dot(
                xf[rows, :], jnp.concatenate([high, low], 0), preferred_element_type=F32
            ) + jnp.dot(xfl[rows, :], high, preferred_element_type=F32)

        return along_x(0, upper + lower), along_x(N, upper - lower)

    def back(half, cosine, sine):
        k = khat[half]
        k = jnp.concatenate([k, k], 1)
        even = dot3((xih[:, :N], xil[:, :N]), split(cosine * k))
        odd = dot3((xih[:, N:], xil[:, N:]), split(sine * k))
        return dot3(split(jnp.concatenate([even + odd, even - odd], 0)), (th[...], tl[...]))

    def send_back(half, cosine, sine):
        target = send_i.at[half]
        for t in range(2):
            lanes = slice(128 * t, 128 * t + 128)
            low, high = exchange_halves(cosine[:, lanes], sine[:, lanes])
            target[512 * t : 512 * t + 256, :] = low
            target[512 * t + 256 : 512 * t + 512, :] = high
        send(target, recv_i.at[half], 3 + half)

    arrived(recv_f.at[0], recv_sem.at[0])
    plane, plane_k = planes(recv_f.at[0])
    transform_kernel(0, plane_k)
    stage[...] = back(0, *ahead(plane))
    arrived(recv_f.at[1], recv_sem.at[1])
    plane, other = planes(recv_f.at[1])
    send_back(0, stage[...], back(0, *ahead(plane)))
    waves[0], waves[1] = ahead(other)
    arrived(recv_f.at[2], recv_sem.at[2])
    plane, plane_k = planes(recv_f.at[2])
    transform_kernel(1, plane_k)
    send_back(1, back(1, waves[0], waves[1]), back(1, *ahead(plane)))

    for half in range(2):
        arrived(recv_i.at[half], recv_sem.at[3 + half])
        source = recv_i.at[half]
        table = tuple(
            jnp.concatenate(
                [r[:, 128 * half : 128 * half + 128], r[:, N + 128 * half : N + 128 * half + 128]], 1
            )
            for r in (tth, ttl)
        )
        for t in range(4):
            a = source[pl.ds(line(2 * t), DEVICES, stride=8), :]
            b = source[pl.ds(line(2 * t + 1), DEVICES, stride=8), :]
            first, second = exchange_halves(a, b)
            waves = split(jnp.concatenate([first, second], 0))
            part = dot3(table, waves)
            if half == 0:
                total[:, 128 * t : 128 * t + 128] = part
            else:
                part = part + total[:, 128 * t : 128 * t + 128]
                out[2 * t : 2 * t + 2] = part.T.reshape(2, 64, N)

    for index in range(5):
        arrived(recv_i.at[0], send_sem.at[index])


def solution(mesh):
    constants = tables()

    def on_device(density, green_octant):
        vmem = pl.BlockSpec(memory_space=pltpu.VMEM)
        operands = [density, green_octant, *[jnp.asarray(t) for t in constants]]
        three = pltpu.VMEM((3, DEVICES * 8, 128), F32)
        two = pltpu.VMEM((2, DEVICES * 8, 128), F32)
        return pl.pallas_call(
            kernel,
            out_shape=pltpu.VMEM((8, 64, N), F32),
            in_specs=[pl.BlockSpec(memory_space=pl.ANY)] * len(operands),
            out_specs=vmem,
            scratch_shapes=[
                *[pltpu.VMEM(o.shape, o.dtype) for o in operands],
                three, three, two, two,
                pltpu.VMEM((2, N, N), F32),
                pltpu.VMEM((N, N), F32),
                pltpu.VMEM((2, N, 2 * N), F32),
                pltpu.VMEM((N, 2 * N), F32),
                pltpu.SemaphoreType.DMA((5,)),
                pltpu.SemaphoreType.DMA((5,)),
                pltpu.SemaphoreType.DMA((len(operands),)),
            ],
            compiler_params=pltpu.CompilerParams(
                collective_id=0, has_side_effects=True, vmem_limit_bytes=56 << 20
            ),
        )(*operands)

    return jax.shard_map(
        on_device,
        mesh=mesh,
        in_specs=(P("row", "col", None), P("row", "col", None)),
        out_specs=P("row", "col", None),
        check_vma=False,
    )
```

```python
import itertools
import random

import jax
import jax.numpy as jnp
import numpy as np
from jax import lax
from jax.experimental import pallas as pl
from jax.experimental.pallas import tpu as pltpu
from jax.sharding import PartitionSpec as P

N = 256
ROWS, COLS = 32, 4
DEVICES = ROWS * COLS
BF16, F32 = jnp.bfloat16, jnp.float32
MESH = pl.DeviceIdType.MESH
DENS, GREEN, TH, TL, TTH, TTL, WH, WL, WTH, WTL, XWH, XWL, XF, XFL, XIH, XIL = range(16)


def steps(offset):
    taken = np.zeros((3, 2))
    for dim, step in enumerate((offset[0], offset[1], offset[3])):
        if step == 2:
            taken[dim] += 1
        elif step:
            taken[dim, step // 2] += 1
    return taken


def send_order(seed, window=40):
    rest = [o for o in itertools.product(range(4), range(4), range(2), range(4)) if any(o)]
    random.Random(seed).shuffle(rest)
    rest.sort(key=lambda o: -sum(min(n, 4 - n) for n in (o[0], o[1], o[3])))
    load, order = np.zeros((3, 2)), []
    while rest:
        best = min(rest[:window], key=lambda o: ((load + steps(o)).max(), (load + steps(o)).var()))
        rest.remove(best)
        load += steps(best)
        order.append(best)
    return order


LATE = (3, 4)
ORDERS = [send_order(5 + chunk) for chunk in range(5)]


def split(value):
    high = value.astype(BF16)
    return high, (value - high.astype(F32)).astype(BF16)


def tables():
    wave = np.arange(N)[:, None]
    cell = np.arange(N)[None, :]
    angle = np.pi * (((2 * wave + 1) * cell) % (4 * N)) / (2 * N)
    frame = np.concatenate([np.cos(angle), np.sin(angle)], axis=0)
    even = np.where(cell == 0, 1.0, 2.0) * np.cos(angle)
    folded = np.concatenate([np.arange(N // 2), np.arange(N - 1, N // 2 - 1, -1)])
    middle = np.pi * (((2 * wave + 1) * (2 * cell[:, : N // 2] - (N - 1))) % (8 * N)) / (4 * N)
    half = np.concatenate([np.cos(middle), np.sin(middle)], axis=0)

    def terms(table):
        high = table.astype(np.float32).astype(BF16)
        return [high, (table - high.astype(np.float64)).astype(np.float32).astype(BF16)]

    out = []
    for table in (frame, frame.T, even, even.T, even[:, folded]):
        out += terms(table)
    high, low = terms(half)
    out += [np.concatenate([high, high], axis=1), low]
    high, low = terms(np.concatenate([np.cos(middle).T, np.sin(middle).T], axis=1))
    return [*out, high, low]


def dot3(a, b, dims=(((1,), (0,)), ((), ()))):
    def one(x, y):
        return lax.dot_general(x, y, dims, preferred_element_type=F32)

    return one(a[0], b[0]) + one(a[0], b[1]) + one(a[1], b[0])


def low_half(shape):
    return lax.broadcasted_iota(jnp.int32, shape, len(shape) - 1) < 64


def exchange_halves(a, b):
    low = low_half(a.shape)
    return (
        jnp.where(low, a, pltpu.roll(b, 64, 1)),
        jnp.where(low, pltpu.roll(a, 64, 1), b),
    )


def kernel(*refs):
    operands, out, refs = refs[:16], refs[16], refs[17:]
    fetched, refs = refs[:16], refs[16:]
    send_f, recv_f, send_i, recv_i, khat, stage, waves, total, send_sem, recv_sem, load_sem = refs
    dens, green, th, tl, tth, ttl, wh, wl, wth, wtl, xwh, xwl, xf, xfl, xih, xil = fetched
    row, z = lax.axis_index("row"), lax.axis_index("col")
    y, x, c = row // 8, (row // 2) % 4, row % 2
    flip = row // 16

    def slot(r, q):
        return q * ROWS + r + (r // 16) * (47 - 2 * r)

    def line(n):
        return n + flip * (7 - 2 * n)

    mine = slot(row, z)

    def partners(chunk=0):
        for dy, dx, dc, dz in ORDERS[chunk]:
            r = (((y + dy) % 4) * 4 + (x + dx) % 4) * 2 + (c + dc) % 2
            yield r, (z + dz) % 4

    barrier = pltpu.get_barrier_semaphore()
    def load(index):
        return pltpu.make_async_copy(operands[index], fetched[index], load_sem.at[index])

    order = (DENS, TH, TL, GREEN, WH, WL, WTH, WTL, XWH, XWL, TTH, TTL, XF, XFL, XIH, XIL)
    for index in order[:3]:
        load(index).start()
    for r, q in partners():
        pl.semaphore_signal(barrier, inc=1, device_id=(r, q), device_id_type=MESH)
    for index in order[3:]:
        load(index).start()

    def tile(ref, index):
        return ref.at[pl.ds(pl.multiple_of(index * 8, 8), 8)]

    def ordered(index):
        if index not in LATE:
            yield from ((r, q, False) for r, q in partners(index))
            return
        for base in (0, 2):
            for dy, dx, dc, dz in ORDERS[index] + [(0, 0, 0, 0)]:
                if dz < 2:
                    r = (((y + dy) % 4) * 4 + (x + dx) % 4) * 2 + (c + dc) % 2
                    yield r, base + (z + dz) % 2, (dy, dx, dc) == (0, 0, 0)

    def send(source, target, index):
        for r, q, near in ordered(index):

            def start(r=r, q=q):
                pltpu.make_async_remote_copy(
                    src_ref=tile(source, slot(r, q)),
                    dst_ref=tile(target, mine),
                    send_sem=send_sem.at[index],
                    recv_sem=recv_sem.at[index],
                    device_id=(r, q),
                    device_id_type=MESH,
                ).start()

            if near:
                pl.when(q != z)(start)
            else:
                start()
        own = pl.ds(pl.multiple_of(mine * 8, 8), 8)
        target[own, :] = source[own, :]

    def arrived(target, sem):
        most = target.at[pl.ds(0, (DEVICES - 1) * 8)]
        pltpu.make_async_copy(most, most, sem).wait()

    def along_z(upper, lower, target):
        def one(pair, t):
            rows = slice(128 * t, 128 * t + 128)
            data = tuple(ref[rows] for ref in pair[1])
            return dot3(pair[0], data, (((1,), (1,)), ((), ())))

        for t in range(4):
            first, second = exchange_halves(one(upper, t), one(lower, t))
            target[pl.ds(line(2 * t), DEVICES, stride=8), :] = first
            target[pl.ds(line(2 * t + 1), DEVICES, stride=8), :] = second

    def rows_of(high, low, start):
        return high[start : start + 128], low[start : start + 128]

    for index in order[:6]:
        load(index).wait()
    g = split(green[...].reshape(8 * 64, N))
    d = split(dens[...].reshape(8 * 64, N))
    along_z((rows_of(th, tl, 0), d), (rows_of(wh, wl, 0), g), send_f.at[0])
    pl.semaphore_wait(barrier, DEVICES - 1)
    send(send_f.at[0], recv_f.at[0], 0)
    along_z((rows_of(th, tl, N), d), (rows_of(th, tl, 128), d), send_f.at[1])
    send(send_f.at[1], recv_f.at[1], 1)
    along_z((rows_of(th, tl, N + 128), d), (rows_of(wh, wl, 128), g), send_f.at[2])
    send(send_f.at[2], recv_f.at[2], 2)
    for index in order[6:]:
        load(index).wait()

    def planes(ref):
        first, second = [], []
        for t in range(2):
            a = ref[512 * t : 512 * t + 256, :]
            b = ref[512 * t + 256 : 512 * t + 512, :]
            low, high = exchange_halves(a, b)
            first.append(low)
            second.append(high)
        return jnp.concatenate(first, 1), jnp.concatenate(second, 1)

    def transform_kernel(half, plane):
        along_y = dot3(split(plane), (wth[...], wtl[...]))
        khat[half] = dot3((xwh[...], xwl[...]), split(along_y)) * F32(1.0 / N**3)

    def ahead(plane):
        along_y = dot3(split(plane), (tth[...], ttl[...]))
        upper, lower = along_y[: N // 2], along_y[N // 2 :]

        def along_x(start, cells):
            high, low = split(cells)
            rows = slice(start, start + N)
            return jnp.dot(
                xf[rows, :], jnp.concatenate([high, low], 0), preferred_element_type=F32
            ) + jnp.dot(xfl[rows, :], high, preferred_element_type=F32)

        return along_x(0, upper + lower), along_x(N, upper - lower)

    def back(half, cosine, sine):
        k = khat[half]
        k = jnp.concatenate([k, k], 1)
        even = dot3((xih[:, :N], xil[:, :N]), split(cosine * k))
        odd = dot3((xih[:, N:], xil[:, N:]), split(sine * k))
        return dot3(split(jnp.concatenate([even + odd, even - odd], 0)), (th[...], tl[...]))

    def send_back(half, cosine, sine):
        target = send_i.at[half]
        for t in range(2):
            lanes = slice(128 * t, 128 * t + 128)
            low, high = exchange_halves(cosine[:, lanes], sine[:, lanes])
            target[512 * t : 512 * t + 256, :] = low
            target[512 * t + 256 : 512 * t + 512, :] = high
        send(target, recv_i.at[half], 3 + half)

    arrived(recv_f.at[0], recv_sem.at[0])
    plane, plane_k = planes(recv_f.at[0])
    transform_kernel(0, plane_k)
    stage[...] = back(0, *ahead(plane))
    arrived(recv_f.at[1], recv_sem.at[1])
    plane, other = planes(recv_f.at[1])
    send_back(0, stage[...], back(0, *ahead(plane)))
    waves[0], waves[1] = ahead(other)
    arrived(recv_f.at[2], recv_sem.at[2])
    plane, plane_k = planes(recv_f.at[2])
    transform_kernel(1, plane_k)
    send_back(1, back(1, waves[0], waves[1]), back(1, *ahead(plane)))

    for half in range(2):
        arrived(recv_i.at[half], recv_sem.at[3 + half])
        source = recv_i.at[half]
        table = tuple(
            jnp.concatenate(
                [r[:, 128 * half : 128 * half + 128], r[:, N + 128 * half : N + 128 * half + 128]], 1
            )
            for r in (tth, ttl)
        )
        for t in range(4):
            a = source[pl.ds(line(2 * t), DEVICES, stride=8), :]
            b = source[pl.ds(line(2 * t + 1), DEVICES, stride=8), :]
            first, second = exchange_halves(a, b)
            waves = split(jnp.concatenate([first, second], 0))
            part = dot3(table, waves)
            if half == 0:
                total[:, 128 * t : 128 * t + 128] = part
            else:
                part = part + total[:, 128 * t : 128 * t + 128]
                out[2 * t : 2 * t + 2] = part.T.reshape(2, 64, N)

    for index in range(5):
        arrived(recv_i.at[0], send_sem.at[index])


def solution(mesh):
    constants = tables()

    def on_device(density, green_octant):
        vmem = pl.BlockSpec(memory_space=pltpu.VMEM)
        operands = [density, green_octant, *[jnp.asarray(t) for t in constants]]
        three = pltpu.VMEM((3, DEVICES * 8, 128), F32)
        two = pltpu.VMEM((2, DEVICES * 8, 128), F32)
        return pl.pallas_call(
            kernel,
            out_shape=pltpu.VMEM((8, 64, N), F32),
            in_specs=[pl.BlockSpec(memory_space=pl.ANY)] * len(operands),
            out_specs=vmem,
            scratch_shapes=[
                *[pltpu.VMEM(o.shape, o.dtype) for o in operands],
                three, three, two, two,
                pltpu.VMEM((2, N, N), F32),
                pltpu.VMEM((N, N), F32),
                pltpu.VMEM((2, N, 2 * N), F32),
                pltpu.VMEM((N, 2 * N), F32),
                pltpu.SemaphoreType.DMA((5,)),
                pltpu.SemaphoreType.DMA((5,)),
                pltpu.SemaphoreType.DMA((len(operands),)),
            ],
            compiler_params=pltpu.CompilerParams(
                collective_id=0, has_side_effects=True, vmem_limit_bytes=56 << 20
            ),
        )(*operands)

    return jax.shard_map(
        on_device,
        mesh=mesh,
        in_specs=(P("row", "col", None), P("row", "col", None)),
        out_specs=P("row", "col", None),
        check_vma=False,
    )
```

```python
import itertools
import random

import jax
import jax.numpy as jnp
import numpy as np
from jax import lax
from jax.experimental import pallas as pl
from jax.experimental.pallas import tpu as pltpu
from jax.sharding import PartitionSpec as P

N = 256
ROWS, COLS = 32, 4
DEVICES = ROWS * COLS
BF16, F32 = jnp.bfloat16, jnp.float32
MESH = pl.DeviceIdType.MESH
DENS, GREEN, TH, TL, TTH, TTL, WH, WL, WTH, WTL, XWH, XWL, XF, XFL, XIH, XIL = range(16)


def steps(offset):
    taken = np.zeros((3, 2))
    for dim, step in enumerate((offset[0], offset[1], offset[3])):
        if step == 2:
            taken[dim] += 1
        elif step:
            taken[dim, step // 2] += 1
    return taken


def send_order(seed, window=40):
    rest = [o for o in itertools.product(range(4), range(4), range(2), range(4)) if any(o)]
    random.Random(seed).shuffle(rest)
    rest.sort(key=lambda o: -sum(min(n, 4 - n) for n in (o[0], o[1], o[3])))
    load, order = np.zeros((3, 2)), []
    while rest:
        best = min(rest[:window], key=lambda o: ((load + steps(o)).max(), (load + steps(o)).var()))
        rest.remove(best)
        load += steps(best)
        order.append(best)
    return order


LATE = (2, 3, 4)
ORDERS = [send_order(5 + chunk) for chunk in range(5)]


def split(value):
    high = value.astype(BF16)
    return high, (value - high.astype(F32)).astype(BF16)


def tables():
    wave = np.arange(N)[:, None]
    cell = np.arange(N)[None, :]
    angle = np.pi * (((2 * wave + 1) * cell) % (4 * N)) / (2 * N)
    frame = np.concatenate([np.cos(angle), np.sin(angle)], axis=0)
    even = np.where(cell == 0, 1.0, 2.0) * np.cos(angle)
    folded = np.concatenate([np.arange(N // 2), np.arange(N - 1, N // 2 - 1, -1)])
    middle = np.pi * (((2 * wave + 1) * (2 * cell[:, : N // 2] - (N - 1))) % (8 * N)) / (4 * N)
    half = np.concatenate([np.cos(middle), np.sin(middle)], axis=0)

    def terms(table):
        high = table.astype(np.float32).astype(BF16)
        return [high, (table - high.astype(np.float64)).astype(np.float32).astype(BF16)]

    out = []
    for table in (frame, frame.T, even, even.T, even[:, folded]):
        out += terms(table)
    high, low = terms(half)
    out += [np.concatenate([high, high], axis=1), low]
    high, low = terms(np.concatenate([np.cos(middle).T, np.sin(middle).T], axis=1))
    return [*out, high, low]


def dot3(a, b, dims=(((1,), (0,)), ((), ()))):
    def one(x, y):
        return lax.dot_general(x, y, dims, preferred_element_type=F32)

    return one(a[0], b[0]) + one(a[0], b[1]) + one(a[1], b[0])


def low_half(shape):
    return lax.broadcasted_iota(jnp.int32, shape, len(shape) - 1) < 64


def exchange_halves(a, b):
    low = low_half(a.shape)
    return (
        jnp.where(low, a, pltpu.roll(b, 64, 1)),
        jnp.where(low, pltpu.roll(a, 64, 1), b),
    )


def kernel(*refs):
    operands, out, refs = refs[:16], refs[16], refs[17:]
    fetched, refs = refs[:16], refs[16:]
    send_f, recv_f, send_i, recv_i, khat, stage, waves, total, send_sem, recv_sem, load_sem = refs
    dens, green, th, tl, tth, ttl, wh, wl, wth, wtl, xwh, xwl, xf, xfl, xih, xil = fetched
    row, z = lax.axis_index("row"), lax.axis_index("col")
    y, x, c = row // 8, (row // 2) % 4, row % 2
    flip = row // 16

    def slot(r, q):
        return q * ROWS + r + (r // 16) * (47 - 2 * r)

    def line(n):
        return n + flip * (7 - 2 * n)

    mine = slot(row, z)

    def partners(chunk=0):
        for dy, dx, dc, dz in ORDERS[chunk]:
            r = (((y + dy) % 4) * 4 + (x + dx) % 4) * 2 + (c + dc) % 2
            yield r, (z + dz) % 4

    barrier = pltpu.get_barrier_semaphore()
    def load(index):
        return pltpu.make_async_copy(operands[index], fetched[index], load_sem.at[index])

    order = (DENS, TH, TL, GREEN, WH, WL, WTH, WTL, XWH, XWL, TTH, TTL, XF, XFL, XIH, XIL)
    for index in order[:3]:
        load(index).start()
    for r, q in partners():
        pl.semaphore_signal(barrier, inc=1, device_id=(r, q), device_id_type=MESH)
    for index in order[3:]:
        load(index).start()

    def tile(ref, index):
        return ref.at[pl.ds(pl.multiple_of(index * 8, 8), 8)]

    def ordered(index):
        if index not in LATE:
            yield from ((r, q, False) for r, q in partners(index))
            return
        for base in (0, 2):
            for dy, dx, dc, dz in ORDERS[index] + [(0, 0, 0, 0)]:
                if dz < 2:
                    r = (((y + dy) % 4) * 4 + (x + dx) % 4) * 2 + (c + dc) % 2
                    yield r, base + (z + dz) % 2, (dy, dx, dc) == (0, 0, 0)

    def send(source, target, index):
        for r, q, near in ordered(index):

            def start(r=r, q=q):
                pltpu.make_async_remote_copy(
                    src_ref=tile(source, slot(r, q)),
                    dst_ref=tile(target, mine),
                    send_sem=send_sem.at[index],
                    recv_sem=recv_sem.at[index],
                    device_id=(r, q),
                    device_id_type=MESH,
                ).start()

            if near:
                pl.when(q != z)(start)
            else:
                start()
        own = pl.ds(pl.multiple_of(mine * 8, 8), 8)
        target[own, :] = source[own, :]

    def arrived(target, sem):
        most = target.at[pl.ds(0, (DEVICES - 1) * 8)]
        pltpu.make_async_copy(most, most, sem).wait()

    def along_z(upper, lower, target):
        def one(pair, t):
            rows = slice(128 * t, 128 * t + 128)
            data = tuple(ref[rows] for ref in pair[1])
            return dot3(pair[0], data, (((1,), (1,)), ((), ())))

        for t in range(4):
            first, second = exchange_halves(one(upper, t), one(lower, t))
            target[pl.ds(line(2 * t), DEVICES, stride=8), :] = first
            target[pl.ds(line(2 * t + 1), DEVICES, stride=8), :] = second

    def rows_of(high, low, start):
        return high[start : start + 128], low[start : start + 128]

    for index in order[:6]:
        load(index).wait()
    g = split(green[...].reshape(8 * 64, N))
    d = split(dens[...].reshape(8 * 64, N))
    along_z((rows_of(th, tl, 0), d), (rows_of(wh, wl, 0), g), send_f.at[0])
    pl.semaphore_wait(barrier, DEVICES - 1)
    send(send_f.at[0], recv_f.at[0], 0)
    along_z((rows_of(th, tl, N), d), (rows_of(th, tl, 128), d), send_f.at[1])
    send(send_f.at[1], recv_f.at[1], 1)
    along_z((rows_of(th, tl, N + 128), d), (rows_of(wh, wl, 128), g), send_f.at[2])
    send(send_f.at[2], recv_f.at[2], 2)
    for index in order[6:]:
        load(index).wait()

    def planes(ref):
        first, second = [], []
        for t in range(2):
            a = ref[512 * t : 512 * t + 256, :]
            b = ref[512 * t + 256 : 512 * t + 512, :]
            low, high = exchange_halves(a, b)
            first.append(low)
            second.append(high)
        return jnp.concatenate(first, 1), jnp.concatenate(second, 1)

    def transform_kernel(half, plane):
        along_y = dot3(split(plane), (wth[...], wtl[...]))
        khat[half] = dot3((xwh[...], xwl[...]), split(along_y)) * F32(1.0 / N**3)

    def ahead(plane):
        along_y = dot3(split(plane), (tth[...], ttl[...]))
        upper, lower = along_y[: N // 2], along_y[N // 2 :]

        def along_x(start, cells):
            high, low = split(cells)
            rows = slice(start, start + N)
            return jnp.dot(
                xf[rows, :], jnp.concatenate([high, low], 0), preferred_element_type=F32
            ) + jnp.dot(xfl[rows, :], high, preferred_element_type=F32)

        return along_x(0, upper + lower), along_x(N, upper - lower)

    def back(half, cosine, sine):
        k = khat[half]
        k = jnp.concatenate([k, k], 1)
        even = dot3((xih[:, :N], xil[:, :N]), split(cosine * k))
        odd = dot3((xih[:, N:], xil[:, N:]), split(sine * k))
        return dot3(split(jnp.concatenate([even + odd, even - odd], 0)), (th[...], tl[...]))

    def send_back(half, cosine, sine):
        target = send_i.at[half]
        for t in range(2):
            lanes = slice(128 * t, 128 * t + 128)
            low, high = exchange_halves(cosine[:, lanes], sine[:, lanes])
            target[512 * t : 512 * t + 256, :] = low
            target[512 * t + 256 : 512 * t + 512, :] = high
        send(target, recv_i.at[half], 3 + half)

    arrived(recv_f.at[0], recv_sem.at[0])
    plane, plane_k = planes(recv_f.at[0])
    transform_kernel(0, plane_k)
    stage[...] = back(0, *ahead(plane))
    arrived(recv_f.at[1], recv_sem.at[1])
    plane, other = planes(recv_f.at[1])
    send_back(0, stage[...], back(0, *ahead(plane)))
    waves[0], waves[1] = ahead(other)
    arrived(recv_f.at[2], recv_sem.at[2])
    plane, plane_k = planes(recv_f.at[2])
    transform_kernel(1, plane_k)
    send_back(1, back(1, waves[0], waves[1]), back(1, *ahead(plane)))

    for half in range(2):
        arrived(recv_i.at[half], recv_sem.at[3 + half])
        source = recv_i.at[half]
        table = tuple(
            jnp.concatenate(
                [r[:, 128 * half : 128 * half + 128], r[:, N + 128 * half : N + 128 * half + 128]], 1
            )
            for r in (tth, ttl)
        )
        for t in range(4):
            a = source[pl.ds(line(2 * t), DEVICES, stride=8), :]
            b = source[pl.ds(line(2 * t + 1), DEVICES, stride=8), :]
            first, second = exchange_halves(a, b)
            waves = split(jnp.concatenate([first, second], 0))
            part = dot3(table, waves)
            if half == 0:
                total[:, 128 * t : 128 * t + 128] = part
            else:
                part = part + total[:, 128 * t : 128 * t + 128]
                out[2 * t : 2 * t + 2] = part.T.reshape(2, 64, N)

    for index in range(5):
        arrived(recv_i.at[0], send_sem.at[index])


def solution(mesh):
    constants = tables()

    def on_device(density, green_octant):
        vmem = pl.BlockSpec(memory_space=pltpu.VMEM)
        operands = [density, green_octant, *[jnp.asarray(t) for t in constants]]
        three = pltpu.VMEM((3, DEVICES * 8, 128), F32)
        two = pltpu.VMEM((2, DEVICES * 8, 128), F32)
        return pl.pallas_call(
            kernel,
            out_shape=pltpu.VMEM((8, 64, N), F32),
            in_specs=[pl.BlockSpec(memory_space=pl.ANY)] * len(operands),
            out_specs=vmem,
            scratch_shapes=[
                *[pltpu.VMEM(o.shape, o.dtype) for o in operands],
                three, three, two, two,
                pltpu.VMEM((2, N, N), F32),
                pltpu.VMEM((N, N), F32),
                pltpu.VMEM((2, N, 2 * N), F32),
                pltpu.VMEM((N, 2 * N), F32),
                pltpu.SemaphoreType.DMA((5,)),
                pltpu.SemaphoreType.DMA((5,)),
                pltpu.SemaphoreType.DMA((len(operands),)),
            ],
            compiler_params=pltpu.CompilerParams(
                collective_id=0, has_side_effects=True, vmem_limit_bytes=56 << 20
            ),
        )(*operands)

    return jax.shard_map(
        on_device,
        mesh=mesh,
        in_specs=(P("row", "col", None), P("row", "col", None)),
        out_specs=P("row", "col", None),
        check_vma=False,
    )
```
